8 devices in a mesh: dp: 2 (over z, y), tp: 4 (over x, core).
Axes of the slice: x: 2, y: 2, z: 1, core: 2. Of those that a mesh axis runs over, the one named last changes fastest.
Arguments:
- x_seq: bfloat16 [24, 512, 5120], P('dp', 'tp'), parts along dimension 0
- ln_gain: float32 [5120], replicated
- ln_bias: float32 [5120], replicated
- w_qkv: bfloat16 [5120, 40, 3, 128], P(None, 'tp')
- w_out: bfloat16 [5120, 5120], P('tp')
- w_up: bfloat16 [5120, 20480], P(None, 'tp')
- w_down: bfloat16 [20480, 5120], P('tp')
Outputs:
- output: bfloat16 [24, 512, 5120], P('dp', 'tp'), parts along dimension 0
There are 2 independent parts. The reference program is written for one: setup_inputs(seed, part) draws one part's arguments, and reference() takes and returns one part's arrays. A program takes and returns all parts, laid end to end along the dimension named above; an argument that names none is the same for every part.
All inputs are finite; a program needn't handle non-finite values.
Results may differ from the reference program's by a relative error of at most 0.00944055.
Values are sent between devices in bfloat16 or wider.
A program may use at most 1 GiB of HBM per device.

```python
import jax
import jax.numpy as jnp
from jax import lax

D = 5120
HEADS = 40
KV_HEADS = 40
HEAD = 128
FF = 20480
BATCH = 12
SEQ = 512

LN_EPS = 1e-5
GROUP_Q = HEADS // KV_HEADS


def normal_weights(key_w, shape, fan_in):
    return (jax.random.normal(key_w, shape, jnp.float32) * fan_in ** -0.5).astype(jnp.bfloat16)


def setup_inputs(seed: int = 0, part: int = 0) -> dict:
    root_key = jax.random.key(seed)
    key_x, key_c, key_g, key_b, key_qkv, key_o, key_up, key_dn = jax.random.split(root_key, 8)
    key_x = jax.random.fold_in(key_x, part)
    key_c = jax.random.fold_in(key_c, part)
    noise = jax.random.normal(key_x, (BATCH, SEQ, D), jnp.float32)
    shared = jax.random.normal(key_c, (BATCH, 1, D), jnp.float32)
    x_seq = ((noise + shared) * 0.7071).astype(jnp.bfloat16)
    ln_gain = 1.0 + 0.5 * jax.random.normal(key_g, (D,), jnp.float32)
    ln_bias = 0.5 * jax.random.normal(key_b, (D,), jnp.float32)
    w_qkv = normal_weights(key_qkv, (D, KV_HEADS, GROUP_Q + 2, HEAD), D)
    w_out = normal_weights(key_o, (HEADS * HEAD, D), HEADS * HEAD)
    w_up = normal_weights(key_up, (D, FF), D)
    w_down = normal_weights(key_dn, (FF, D), FF)
    return {"x_seq": x_seq, "ln_gain": ln_gain, "ln_bias": ln_bias, "w_qkv": w_qkv,
            "w_out": w_out, "w_up": w_up, "w_down": w_down}


def layer_norm(x_f32, ln_gain, ln_bias):
    row_mean = jnp.mean(x_f32, axis=-1, keepdims=True)
    centered = x_f32 - row_mean
    variance = jnp.mean(centered * centered, axis=-1, keepdims=True)
    return centered * lax.rsqrt(variance + LN_EPS) * ln_gain + ln_bias


def reference(x_seq, ln_gain, ln_bias, w_qkv, w_out, w_up, w_down):
    tokens = x_seq.reshape(BATCH * SEQ, D)
    normed = layer_norm(tokens.astype(jnp.float32), ln_gain, ln_bias).astype(jnp.bfloat16)
    proj_qkv = jnp.dot(normed, w_qkv.reshape(D, KV_HEADS * (GROUP_Q + 2) * HEAD),
                       preferred_element_type=jnp.float32).astype(jnp.bfloat16)
    proj_qkv = proj_qkv.reshape(BATCH, SEQ, KV_HEADS, GROUP_Q + 2, HEAD)
    proj_qkv = proj_qkv.transpose(0, 2, 3, 1, 4).reshape(BATCH * KV_HEADS, GROUP_Q + 2, SEQ, HEAD)
    causal = jnp.arange(SEQ)[:, None] >= jnp.arange(SEQ)[None, :]

    def one_group(group_item):
        query_rows = group_item[:GROUP_Q].astype(jnp.float32)
        key_rows = group_item[GROUP_Q].astype(jnp.float32)
        value_rows = group_item[GROUP_Q + 1].astype(jnp.float32)
        scores = jnp.einsum("jsh,th->jst", query_rows, key_rows) * (HEAD ** -0.5)
        scores = jnp.where(causal, scores, -jnp.inf)
        attn_prob = jax.nn.softmax(scores, axis=-1).astype(jnp.bfloat16)
        context = jnp.einsum("jst,th->jsh", attn_prob.astype(jnp.float32), value_rows)
        return context.astype(jnp.bfloat16)

    context = lax.map(one_group, proj_qkv)
    context = context.reshape(BATCH, KV_HEADS, GROUP_Q, SEQ, HEAD).transpose(0, 3, 1, 2, 4)
    context = context.reshape(BATCH * SEQ, HEADS * HEAD)
    attn_part = jnp.dot(context, w_out, preferred_element_type=jnp.float32)
    hidden = jnp.dot(normed, w_up, preferred_element_type=jnp.float32)
    activated = jax.nn.gelu(hidden, approximate=False).astype(jnp.bfloat16)
    mlp_part = jnp.dot(activated, w_down, preferred_element_type=jnp.float32)
    branch = (attn_part + mlp_part).astype(jnp.bfloat16)
    out_rows = (tokens.astype(jnp.float32) + branch.astype(jnp.float32)).astype(jnp.bfloat16)
    return out_rows.reshape(BATCH, SEQ, D)
```

```python
import functools

import jax
import jax.numpy as jnp
from jax import lax
from jax.experimental import pallas as pl
from jax.experimental.pallas import tpu as pltpu
from jax.sharding import PartitionSpec as P

LN_EPS = 1e-5
BF = jnp.bfloat16
F32 = jnp.float32
MESH = pl.DeviceIdType.MESH
ANY = pl.BlockSpec(memory_space=pl.ANY)
VMEM_LIMIT = 66_000_000


def ds(i, n):
    return pl.ds(pl.multiple_of(i * n, n), n)


def neighbours():
    t = lax.axis_index("tp")
    c = t % 2
    sib = t + 1 - 2 * c
    far = (t + 2) % 4
    far_sib = (sib + 2) % 4
    return t, sib, far, far_sib


def meet(sib, far):
    barrier = pltpu.get_barrier_semaphore()
    for peer in (sib, far):
        pl.semaphore_signal(barrier, inc=1, device_id={"tp": peer}, device_id_type=MESH)
    pl.semaphore_wait(barrier, 2)


def send(src, dst, send_sem, recv_sem, peer):
    return pltpu.make_async_remote_copy(src_ref=src, dst_ref=dst, send_sem=send_sem, recv_sem=recv_sem,
                                        device_id={"tp": peer}, device_id_type=MESH)


def ln_body(x_ref, g_ref, b_ref, o_ref):
    x = x_ref[...].astype(F32)
    mean = jnp.mean(x, axis=-1, keepdims=True)
    cen = x - mean
    var = jnp.mean(cen * cen, axis=-1, keepdims=True)
    o_ref[...] = (cen * lax.rsqrt(var + LN_EPS) * g_ref[...] + b_ref[...]).astype(BF)


def ln_call(x, gain, bias, rows=128):
    m, d = x.shape
    return pl.pallas_call(
        ln_body, grid=(m // rows,),
        in_specs=[pl.BlockSpec((rows, d), lambda i: (i, 0)), pl.BlockSpec((1, d), lambda i: (0, 0)),
                  pl.BlockSpec((1, d), lambda i: (0, 0))],
        out_specs=pl.BlockSpec((rows, d), lambda i: (i, 0)),
        out_shape=jax.ShapeDtypeStruct((m, d), BF),
        compiler_params=pltpu.CompilerParams(vmem_limit_bytes=VMEM_LIMIT), name="ln")(x, gain, bias)


def enter_body(n_ref, wq_ref, wu_ref, qkv_ref, h_ref, in_ref, lhs, wq, wu, oq, ou,
               lhs_sem, wq_sem, wu_sem, oq_sem, ou_sem, ssem, rsem, *, M, TQ, TU, NQ, NU):
    t, sib, far, far_sib = neighbours()
    meet(sib, far)
    half = n_ref.shape[0] // 2
    heads = TQ // 384

    def part(ref, k):
        return ref.at[pl.ds(k * half, half), :]

    far_cp = [send(part(n_ref, k), in_ref.at[1, pl.ds(k * half, half), :], ssem.at[k], rsem.at[k], far) for k in (0, 1)]
    sib_cp = [send(part(n_ref, k), in_ref.at[0, pl.ds(k * half, half), :], ssem.at[2 + k], rsem.at[2 + k], sib)
              for k in (0, 1)]
    fwd_cp = [send(in_ref.at[1, pl.ds(k * half, half), :], in_ref.at[2, pl.ds(k * half, half), :], ssem.at[4 + k],
                   rsem.at[4 + k], sib) for k in (0, 1)]

    def wq_copies(j, slot):
        return [pltpu.make_async_copy(wq_ref.at[j * heads + i, k], wq.at[slot, :, pl.ds((i * 3 + k) * 128, 128)],
                                      wq_sem.at[slot, i * 3 + k]) for i in range(heads) for k in range(3)]

    def wu_copy(j, slot):
        return pltpu.make_async_copy(wu_ref.at[:, ds(j, TU)], wu.at[slot], wu_sem.at[slot])

    def own_lhs(k, slot):
        return pltpu.make_async_copy(n_ref.at[ds(k, M), :], lhs.at[slot], lhs_sem.at[slot])

    def in_lhs(which, k, slot):
        return pltpu.make_async_copy(in_ref.at[which, ds(k, M), :], lhs.at[slot], lhs_sem.at[slot])

    for cp in (far_cp[0], sib_cp[0], sib_cp[1], far_cp[1]):
        cp.start()
    own_lhs(0, 0).start()
    for cp in wq_copies(0, 0):
        cp.start()

    def block(b, _):
        ls = lax.rem(b, 2)
        k = jnp.where(b < 4, lax.rem(b, 2), (b - 4) // 2)
        which = jnp.where(b < 4, b // 2, 2 + lax.rem(b, 2))
        pos = jnp.where(which == 0, t, jnp.where(which == 1, sib, jnp.where(which == 2, far, far_sib)))
        pltpu.make_async_copy(n_ref.at[pl.ds(0, M), :], lhs.at[ls], lhs_sem.at[ls]).wait()

        def q_step(j, _):
            g = b * NQ + j
            slot = lax.rem(g, 2)
            for cp in wq_copies(j, slot):
                cp.wait()

            @pl.when(j < NQ - 1)
            def _():
                for cp in wq_copies(j + 1, 1 - slot):
                    cp.start()

            @pl.when(j == NQ - 1)
            def _():
                wu_copy(0, 0).start()

            @pl.when(g >= 2)
            def _():
                pltpu.make_async_copy(oq.at[slot], qkv_ref.at[0, pl.ds(0, M), pl.ds(0, TQ)], oq_sem.at[slot]).wait()
            oq[slot] = jnp.dot(lhs[ls], wq[slot], preferred_element_type=F32).astype(BF)
            pltpu.make_async_copy(oq.at[slot], qkv_ref.at[pos, ds(k, M), ds(j, TQ)], oq_sem.at[slot]).start()
            return 0

        lax.fori_loop(0, NQ, q_step, 0)

        def u_step(j, _):
            slot = lax.rem(j, 2)
            wu_copy(j, slot).wait()

            @pl.when(j < NU - 1)
            def _():
                wu_copy(j + 1, 1 - slot).start()

            @pl.when((j == NU - 1) & (b < 7))
            def _():
                for cp in wq_copies(0, lax.rem((b + 1) * NQ, 2)):
                    cp.start()

            @pl.when(j == NU // 2)
            def _():
                nxt = 1 - ls

                @pl.when(b == 0)
                def _():
                    own_lhs(1, nxt).start()

                for bb, kk in ((1, 0), (2, 1)):
                    @pl.when(b == bb)
                    def _():
                        sib_cp[kk].wait_recv()
                        in_lhs(0, kk, nxt).start()

                for bb, kk in ((3, 0), (5, 1)):
                    @pl.when(b == bb)
                    def _():
                        far_cp[kk].wait_recv()
                        fwd_cp[kk].start()
                        in_lhs(1, kk, nxt).start()

                for bb, kk in ((4, 0), (6, 1)):
                    @pl.when(b == bb)
                    def _():
                        fwd_cp[kk].wait_recv()
                        in_lhs(2, kk, nxt).start()

            @pl.when((b > 0) | (j >= 2))
            def _():
                pltpu.make_async_copy(ou.at[slot], h_ref.at[0, pl.ds(0, M), pl.ds(0, TU)], ou_sem.at[slot]).wait()
            z = jnp.dot(lhs[ls], wu[slot], preferred_element_type=F32)
            ou[slot] = (z * 0.5 * (1.0 + lax.erf(z * 0.7071067811865476))).astype(BF)
            pltpu.make_async_copy(ou.at[slot], h_ref.at[which, ds(k, M), ds(j, TU)], ou_sem.at[slot]).start()
            return 0

        lax.fori_loop(0, NU, u_step, 0)
        return 0

    lax.fori_loop(0, 8, block, 0)
    for s in (0, 1):
        pltpu.make_async_copy(oq.at[s], qkv_ref.at[0, pl.ds(0, M), pl.ds(0, TQ)], oq_sem.at[s]).wait()
        pltpu.make_async_copy(ou.at[s], h_ref.at[0, pl.ds(0, M), pl.ds(0, TU)], ou_sem.at[s]).wait()
    for cp in far_cp + sib_cp + fwd_cp:
        cp.wait_send()


def enter_call(n, wq, wu):
    rows, d = n.shape
    M, TQ, TU = rows // 2, 768, 512
    cq, cu = wq.shape[0] * 384, wu.shape[1]
    NQ, NU = cq // TQ, cu // TU
    return pl.pallas_call(
        functools.partial(enter_body, M=M, TQ=TQ, TU=TU, NQ=NQ, NU=NU),
        in_specs=[ANY] * 3, out_specs=[ANY] * 3,
        out_shape=[jax.ShapeDtypeStruct((4, rows, cq), BF), jax.ShapeDtypeStruct((4, rows, cu), BF),
                   jax.ShapeDtypeStruct((3, rows, d), BF)],
        scratch_shapes=[pltpu.VMEM((2, M, d), BF), pltpu.VMEM((2, d, TQ), BF), pltpu.VMEM((2, d, TU), BF),
                        pltpu.VMEM((2, M, TQ), BF), pltpu.VMEM((2, M, TU), BF),
                        pltpu.SemaphoreType.DMA((2,)), pltpu.SemaphoreType.DMA((2, TQ // 128)),
                        pltpu.SemaphoreType.DMA((2,)), pltpu.SemaphoreType.DMA((2,)), pltpu.SemaphoreType.DMA((2,)),
                        pltpu.SemaphoreType.DMA((6,)), pltpu.SemaphoreType.DMA((6,))],
        compiler_params=pltpu.CompilerParams(collective_id=0, has_side_effects=True, vmem_limit_bytes=VMEM_LIMIT),
        name="enter")(n, wq, wu)


def attend_body(qkv_ref, o_ref, *, heads, scale):
    Q = 256
    c = scale * 1.4426950408889634
    keep = (lax.broadcasted_iota(jnp.int32, (Q, Q), 0) >= lax.broadcasted_iota(jnp.int32, (Q, Q), 1))

    def probs(s):
        m = jnp.max(s, axis=-1, keepdims=True)
        p = jnp.exp2((s - m) * c)
        return (p * (1.0 / jnp.sum(p, axis=-1, keepdims=True))).astype(BF)

    def head(g):
        def grab(i, j):
            col = pl.ds(pl.multiple_of(g * 384 + j * 128, 128), 128)
            return qkv_ref[2 * i:2 * i + 2, 0, :, col].reshape(Q, 128)
        q = [grab(i, 0) for i in (0, 1)]
        k = [grab(i, 1) for i in (0, 1)]
        v = [grab(i, 2) for i in (0, 1)]
        dn = (((1,), (1,)), ((), ()))
        s00 = lax.dot_general(q[0], k[0], dn, preferred_element_type=F32)
        s10 = lax.dot_general(q[1], k[0], dn, preferred_element_type=F32)
        s11 = lax.dot_general(q[1], k[1], dn, preferred_element_type=F32)
        p0 = probs(jnp.where(keep, s00, -jnp.inf))
        p1 = probs(jnp.concatenate([s10, jnp.where(keep, s11, -jnp.inf)], axis=1))
        o0 = jnp.dot(p0, v[0], preferred_element_type=F32)
        o1 = jnp.dot(p1, jnp.concatenate(v, axis=0), preferred_element_type=F32)
        col = pl.ds(pl.multiple_of(g * 128, 128), 128)
        o_ref[0:2, 0, :, col] = o0.astype(BF).reshape(2, 128, 128)
        o_ref[2:4, 0, :, col] = o1.astype(BF).reshape(2, 128, 128)

    @pl.loop(0, heads // 2)
    def _(i):
        head(2 * i)
        head(2 * i + 1)


def attend_call(qkv, heads):
    _, b, s, cq = qkv.shape
    return pl.pallas_call(
        functools.partial(attend_body, heads=heads, scale=128 ** -0.5), grid=(b,),
        in_specs=[pl.BlockSpec((4, 1, s, cq), lambda i: (0, i, 0, 0))],
        out_specs=pl.BlockSpec((4, 1, s, heads * 128), lambda i: (0, i, 0, 0)),
        out_shape=jax.ShapeDtypeStruct((4, b, s, heads * 128), BF),
        compiler_params=pltpu.CompilerParams(vmem_limit_bytes=VMEM_LIMIT), name="attend")(qkv)


def leave_body(c_ref, h_ref, wo_ref, wd_ref, x_ref, y_ref, out_d2d, out_ici, in_ro, in_sib, in_ici,
               lc, lh, wo, wd, stage, ra, rb, xs,
               lc_sem, lh_sem, wo_sem, wd_sem, st_sem, ra_sem, rb_sem, xs_sem,
               s_ro, r_ro, s_sib, r_sib, s_ici, r_ici, *, M, T, N):
    t, sib, far, far_sib = neighbours()
    meet(sib, far)

    def w_copies(j, slot):
        return (pltpu.make_async_copy(wo_ref.at[:, ds(j, T)], wo.at[slot], wo_sem.at[slot]),
                pltpu.make_async_copy(wd_ref.at[:, ds(j, T)], wd.at[slot], wd_sem.at[slot]))

    def l_copies(pos, rel, k, slot):
        return (pltpu.make_async_copy(c_ref.at[pos, ds(k, M), :], lc.at[slot], lc_sem.at[slot]),
                pltpu.make_async_copy(h_ref.at[rel, ds(k, M), :], lh.at[slot], lh_sem.at[slot]))

    def start(cps):
        for cp in cps:
            cp.start()

    def ro_send(k, j):
        return send(out_d2d.at[0, k, j], in_ro.at[k, j], s_ro.at[k, j], r_ro.at[k, j], sib)

    def sib_send(k, j):
        return send(out_d2d.at[1, k, j], in_sib.at[k, j], s_sib.at[k, j], r_sib.at[k, j], sib)

    def ici_send(k, j):
        return send(out_ici.at[k, j], in_ici.at[k, j], s_ici.at[k, j], r_ici.at[k, j], far)

    def put(kind, k, j, slot):
        if kind == "own":
            dst = y_ref.at[ds(k, M), ds(j, T)]
        elif kind == "rs":
            dst = out_ici.at[k, j]
        else:
            dst = out_d2d.at[0 if kind == "ro" else 1, k, j]
        return pltpu.make_async_copy(stage.at[slot], dst, st_sem.at[slot])

    remote = {"ro": ro_send, "rs": ici_send, "sib": sib_send}
    rel_of = {"own": 0, "sib": 1, "rs": 2, "ro": 3}
    pos_of = {"own": t, "sib": sib, "rs": far, "ro": far_sib}

    def adds(kind, k, j, slot):
        if kind == "rs":
            ro_send(k, j).wait_recv()
            pltpu.make_async_copy(in_ro.at[k, j], ra.at[slot], ra_sem.at[slot]).start()
        if kind == "own":
            sib_send(k, j).wait_recv()
            ici_send(k, j).wait_recv()
            pltpu.make_async_copy(in_sib.at[k, j], ra.at[slot], ra_sem.at[slot]).start()
            pltpu.make_async_copy(in_ici.at[k, j], rb.at[slot], rb_sem.at[slot]).start()
            pltpu.make_async_copy(x_ref.at[ds(k, M), ds(j, T)], xs.at[slot], xs_sem.at[slot]).start()

    def run(kind, k, ls, nxt, prev):
        for cp in l_copies(0, 0, 0, ls):
            cp.wait()

        def step(j, _):
            slot = lax.rem(j, 2)
            for cp in w_copies(j, slot):
                cp.wait()

            @pl.when(j < N - 1)
            def _():
                start(w_copies(j + 1, 1 - slot))
                adds(kind, k, j + 1, 1 - slot)

            if nxt is not None:
                for nk, nh, cond in nxt:
                    @pl.when((j == N - 1) & cond)
                    def _():
                        start(w_copies(0, 0))
                        adds(nk, nh, 0, 0)

                    @pl.when((j == N // 2) & cond)
                    def _():
                        start(l_copies(pos_of[nk], rel_of[nk], nh, 1 - ls))

            if kind in ("rs", "own"):
                pltpu.make_async_copy(in_ro.at[0, 0], ra.at[slot], ra_sem.at[slot]).wait()
            if kind == "own":
                pltpu.make_async_copy(in_ici.at[0, 0], rb.at[slot], rb_sem.at[slot]).wait()
                pltpu.make_async_copy(x_ref.at[pl.ds(0, M), pl.ds(0, T)], xs.at[slot], xs_sem.at[slot]).wait()
            z = (jnp.dot(lc[ls], wo[slot], preferred_element_type=F32)
                 + jnp.dot(lh[ls], wd[slot], preferred_element_type=F32))
            if kind == "rs":
                z = z + ra[slot].astype(F32)
            if kind == "own":
                z = (z + ra[slot].astype(F32)) + rb[slot].astype(F32)
                z = xs[slot].astype(F32) + z.astype(BF).astype(F32)
            stage[slot] = z.astype(BF)

            @pl.when(j > 0)
            def _():
                put(kind, k, j - 1, 1 - slot).wait()
                if kind != "own":
                    remote[kind](k, j - 1).start()

            for pk, ph, cond in prev:
                @pl.when((j == 0) & cond)
                def _():
                    put(pk, ph, N - 1, 1).wait()
                    if pk != "own":
                        remote[pk](ph, N - 1).start()
            put(kind, k, j, slot).start()
            return 0

        lax.fori_loop(0, N, step, 0)

    start(w_copies(0, 0))
    start(l_copies(pos_of["ro"], rel_of["ro"], 0, 0))

    def pair(p, _):
        run("ro", p, 0, [("rs", p, p >= 0)], [("rs", p - 1, p > 0)])
        run("rs", p, 1, [("ro", p + 1, p == 0), ("sib", 0, p == 1)], [("ro", p, p >= 0)])
        return 0

    lax.fori_loop(0, 2, pair, 0)

    def sib_pair(p, _):
        run("sib", p, lax.rem(p, 2), [("sib", p + 1, p == 0), ("own", 0, p == 1)], [("rs", 1, p == 0), ("sib", p - 1, p > 0)])
        return 0

    lax.fori_loop(0, 2, sib_pair, 0)

    def own_pair(p, _):
        run("own", p, lax.rem(p, 2), [("own", p + 1, p == 0)], [("sib", 1, p == 0), ("own", p - 1, p > 0)])
        return 0

    lax.fori_loop(0, 2, own_pair, 0)
    put("own", 1, N - 1, 1).wait()

    def drain(i, _):
        k, j = i // N, lax.rem(i, N)
        ro_send(k, j).wait_send()
        sib_send(k, j).wait_send()
        ici_send(k, j).wait_send()
        return 0

    lax.fori_loop(0, 2 * N, drain, 0)


def leave_call(ctx, h, wo, wd, x):
    rows, d = x.shape
    M, T = rows // 2, 512
    N = d // T
    kc, kh = ctx.shape[2], h.shape[2]
    tile = (2, N, M, T)
    dma = pltpu.SemaphoreType.DMA
    out = pl.pallas_call(
        functools.partial(leave_body, M=M, T=T, N=N),
        in_specs=[ANY] * 5, out_specs=[ANY] * 6,
        out_shape=[jax.ShapeDtypeStruct((rows, d), BF), jax.ShapeDtypeStruct((2,) + tile, BF)]
        + [jax.ShapeDtypeStruct(tile, BF)] * 4,
        scratch_shapes=[pltpu.VMEM((2, M, kc), BF), pltpu.VMEM((2, M, kh), BF), pltpu.VMEM((2, kc, T), BF),
                        pltpu.VMEM((2, kh, T), BF)] + [pltpu.VMEM((2, M, T), BF)] * 4
        + [dma((2,))] * 8 + [dma((2, N))] * 6,
        compiler_params=pltpu.CompilerParams(collective_id=1, has_side_effects=True, vmem_limit_bytes=VMEM_LIMIT),
        name="leave")(ctx, h, wo, wd, x)
    return out[0]


def solution(mesh):
    def local_layer(x_blk, ln_gain, ln_bias, w_qkv, w_out, w_up, w_down):
        b, s, d = x_blk.shape
        heads = w_qkv.shape[1]
        x = x_blk.reshape(b * s, d)
        n = ln_call(x, ln_gain.reshape(1, d), ln_bias.reshape(1, d))
        qkv, h, _ = enter_call(n, w_qkv.transpose(1, 2, 0, 3), w_up)
        ctx = attend_call(qkv.reshape(4, b, s, -1), heads)
        y = leave_call(ctx.reshape(4, b * s, -1), h, w_out, w_down, x)
        return y.reshape(b, s, d)

    return jax.shard_map(
        local_layer, mesh=mesh,
        in_specs=(P("dp", "tp", None), P(), P(), P(None, "tp", None, None),
                  P("tp", None), P(None, "tp"), P("tp", None)),
        out_specs=P("dp", "tp", None), check_vma=False)
```

```python
import functools

import jax
import jax.numpy as jnp
from jax import lax
from jax.experimental import pallas as pl
from jax.experimental.pallas import tpu as pltpu
from jax.sharding import PartitionSpec as P

LN_EPS = 1e-5
BF = jnp.bfloat16
F32 = jnp.float32
MESH = pl.DeviceIdType.MESH
ANY = pl.BlockSpec(memory_space=pl.ANY)
VMEM_LIMIT = 66_000_000


def ds(i, n):
    return pl.ds(pl.multiple_of(i * n, n), n)


def neighbours():
    t = lax.axis_index("tp")
    c = t % 2
    sib = t + 1 - 2 * c
    far = (t + 2) % 4
    far_sib = (sib + 2) % 4
    return t, sib, far, far_sib


def meet(sib, far):
    barrier = pltpu.get_barrier_semaphore()
    for peer in (sib, far):
        pl.semaphore_signal(barrier, inc=1, device_id={"tp": peer}, device_id_type=MESH)
    pl.semaphore_wait(barrier, 2)


def send(src, dst, send_sem, recv_sem, peer):
    return pltpu.make_async_remote_copy(src_ref=src, dst_ref=dst, send_sem=send_sem, recv_sem=recv_sem,
                                        device_id={"tp": peer}, device_id_type=MESH)


def enter_body(x_ref, g_ref, b_ref, wq_ref, wu_ref, qkv_ref, h_ref, n_ref, in_ref, lhs, w, o, xb,
               lhs_sem, w_sem, o_sem, x_sem, n_sem, ssem, rsem, *, M, T, NQ, NU):
    t, sib, far, far_sib = neighbours()
    steps = NQ + NU
    R, G = xb.shape[1], 16
    d = x_ref.shape[1]

    def half(ref, k):
        return ref.at[pl.ds(k * M, M), :]

    far_cp = [send(half(n_ref, k), half(in_ref.at[1], k), ssem.at[k], rsem.at[k], far) for k in (0, 1)]
    sib_cp = [send(half(n_ref, k), half(in_ref.at[0], k), ssem.at[2 + k], rsem.at[2 + k], sib) for k in (0, 1)]
    fwd_cp = [send(half(in_ref.at[1], k), half(in_ref.at[2], k), ssem.at[4 + k], rsem.at[4 + k], sib) for k in (0, 1)]

    def start_wq(j, slot):
        for i in range(T // 128):
            pltpu.make_async_copy(wq_ref.at[j * (T // 128) + i], w.at[slot, :, pl.ds(i * 128, 128)], w_sem.at[slot]).start()

    def wu_copy(j, slot):
        return pltpu.make_async_copy(wu_ref.at[:, ds(j, T)], w.at[slot], w_sem.at[slot])

    def in_lhs(which, k, slot):
        return pltpu.make_async_copy(in_ref.at[which, ds(k, M), :], lhs.at[slot], lhs_sem.at[slot])

    def x_copy(i, slot):
        return pltpu.make_async_copy(x_ref.at[ds(i, R), :], xb.at[slot], x_sem.at[slot])

    def n_copy(i):
        k, r = i // (M // R), lax.rem(i, M // R)
        return pltpu.make_async_copy(lhs.at[k, ds(r, R), :], n_ref.at[ds(i, R), :], n_sem.at[k])

    def leave_home(k):
        pltpu.make_async_copy(lhs.at[k], half(n_ref, k), n_sem.at[k]).wait()
        far_cp[k].start()
        sib_cp[k].start()

    x_copy(0, 0).start()
    start_wq(0, 0)
    meet(sib, far)

    def normalize(i, _):
        slot = lax.rem(i, 2)
        x_copy(i, slot).wait()

        @pl.when(i < 2 * M // R - 1)
        def _():
            x_copy(i + 1, 1 - slot).start()

        def rows(g, _):
            for u in range(2):
                r = pl.multiple_of((2 * g + u) * G, G)
                v = xb[slot, pl.ds(r, G), :].astype(F32)
                v = v - jnp.sum(v, axis=-1, keepdims=True) * (1.0 / d)
                rstd = lax.rsqrt(jnp.sum(v * v, axis=-1, keepdims=True) * (1.0 / d) + LN_EPS)
                lhs[i // (M // R), pl.ds(pl.multiple_of(lax.rem(i, M // R) * R + r, G), G), :] = (
                    v * rstd * g_ref[...] + b_ref[...]).astype(BF)
            return 0

        lax.fori_loop(0, R // (2 * G), rows, 0)
        n_copy(i).start()

        @pl.when(i == M // R)
        def _():
            leave_home(0)
        return 0

    lax.fori_loop(0, 2 * M // R, normalize, 0)

    def block(b, _):
        ls = lax.rem(b, 2)
        k = jnp.where(b < 4, lax.rem(b, 2), (b - 4) // 2)
        which = jnp.where(b < 4, b // 2, 2 + lax.rem(b, 2))
        pos = jnp.where(which == 0, t, jnp.where(which == 1, sib, jnp.where(which == 2, far, far_sib)))

        @pl.when(b >= 2)
        def _():
            in_lhs(0, 0, ls).wait()

        def begin(j, slot):
            wu_copy(0, slot).wait()

            @pl.when(j < NQ - 1)
            def _():
                start_wq(j + 1, 1 - slot)

            @pl.when((j >= NQ - 1) & (j < steps - 1))
            def _():
                wu_copy(j + 1 - NQ, 1 - slot).start()

            @pl.when((j == steps - 1) & (b < 7))
            def _():
                start_wq(0, 1 - slot)

            @pl.when((b > 0) | (j >= 2))
            def _():
                pltpu.make_async_copy(o.at[slot], h_ref.at[0, pl.ds(0, M), pl.ds(0, T)], o_sem.at[slot]).wait()

        def q_step(j, _):
            slot = lax.rem(b * steps + j, 2)
            begin(j, slot)

            @pl.when((b == 0) & (j == 1))
            def _():
                leave_home(1)
            o[slot] = jnp.dot(lhs[ls], w[slot], preferred_element_type=F32).astype(BF)
            pltpu.make_async_copy(o.at[slot], qkv_ref.at[pos, ds(k, M), ds(j, T)], o_sem.at[slot]).start()
            return 0

        lax.fori_loop(0, NQ, q_step, 0)

        def u_step(j, _):
            slot = lax.rem(b * steps + NQ + j, 2)
            begin(NQ + j, slot)

            @pl.when(j == NU // 2)
            def _():
                nxt = 1 - ls

                for bb, kk in ((1, 0), (2, 1)):
                    @pl.when(b == bb)
                    def _():
                        sib_cp[kk].wait_recv()
                        in_lhs(0, kk, nxt).start()

                for bb, kk in ((3, 0), (5, 1)):
                    @pl.when(b == bb)
                    def _():
                        far_cp[kk].wait_recv()
                        fwd_cp[kk].start()
                        in_lhs(1, kk, nxt).start()

                for bb, kk in ((4, 0), (6, 1)):
                    @pl.when(b == bb)
                    def _():
                        fwd_cp[kk].wait_recv()
                        in_lhs(2, kk, nxt).start()

            z = jnp.dot(lhs[ls], w[slot], preferred_element_type=F32)
            o[slot] = (z * 0.5 * (1.0 + lax.erf(z * 0.7071067811865476))).astype(BF)
            pltpu.make_async_copy(o.at[slot], h_ref.at[which, ds(k, M), ds(j, T)], o_sem.at[slot]).start()
            return 0

        lax.fori_loop(0, NU, u_step, 0)
        return 0

    lax.fori_loop(0, 8, block, 0)
    for s in (0, 1):
        pltpu.make_async_copy(o.at[s], h_ref.at[0, pl.ds(0, M), pl.ds(0, T)], o_sem.at[s]).wait()
    for cp in far_cp + sib_cp + fwd_cp:
        cp.wait_send()


def enter_call(x, gain, bias, wq, wu):
    rows, d = x.shape
    M, T = rows // 2, 1280
    cq, cu = wq.shape[0] * 128, wu.shape[1]
    dma = pltpu.SemaphoreType.DMA
    whole = pl.BlockSpec(memory_space=pltpu.VMEM)
    out = pl.pallas_call(
        functools.partial(enter_body, M=M, T=T, NQ=cq // T, NU=cu // T),
        in_specs=[ANY, whole, whole, ANY, ANY], out_specs=[ANY] * 4,
        out_shape=[jax.ShapeDtypeStruct((4, rows, cq), BF), jax.ShapeDtypeStruct((4, rows, cu), BF),
                   jax.ShapeDtypeStruct((rows, d), BF), jax.ShapeDtypeStruct((3, rows, d), BF)],
        scratch_shapes=[pltpu.VMEM((2, M, d), BF), pltpu.VMEM((2, d, T), BF), pltpu.VMEM((2, M, T), BF),
                        pltpu.VMEM((2, 128, d), BF),
                        dma((2,)), dma((2,)), dma((2,)), dma((2,)), dma((2,)), dma((6,)), dma((6,))],
        compiler_params=pltpu.CompilerParams(collective_id=0, has_side_effects=True, vmem_limit_bytes=VMEM_LIMIT),
        name="enter")(x, gain, bias, wq, wu)
    return out[0], out[1]


def attend_body(qkv_ref, o_ref, *, heads, scale):
    Q = 256
    B = Q // 128
    c = scale * 1.4426950408889634
    keep = (lax.broadcasted_iota(jnp.int32, (Q, Q), 0) <= lax.broadcasted_iota(jnp.int32, (Q, Q), 1))

    def grab(g, i, n, j):
        return qkv_ref[i:i + n, 0, :, g * 384 + j * 128:g * 384 + j * 128 + 128].reshape(n * 128, 128)

    def scores(g, i):
        return lax.dot_general(grab(g, 0, B * (i + 1), 1), grab(g, B * i, B, 0), (((1,), (1,)), ((), ())),
                               preferred_element_type=F32)

    def probs(s, i):
        tail = jnp.where(keep, s[Q * i:], -jnp.inf)
        s = tail if i == 0 else jnp.concatenate([s[:Q * i], tail], axis=0)
        p = jnp.exp2((s - jnp.max(s, axis=0, keepdims=True)) * c)
        return (p * (1.0 / jnp.sum(p, axis=0, keepdims=True))).astype(BF)

    def out(g, i, p):
        o = lax.dot_general(grab(g, 0, B * (i + 1), 2), p, (((0,), (0,)), ((), ())), preferred_element_type=F32)
        o_ref[B * i:B * i + B, 0, :, g * 128:g * 128 + 128] = o.T.astype(BF).reshape(B, 128, 128)

    ahead, behind = 3, 2
    units = [(g, i) for g in range(heads) for i in range(4 // B)]
    s = {n: scores(*units[n]) for n in range(ahead)}
    p = {}
    for n, (g, i) in enumerate(units):
        if n + ahead < len(units):
            s[n + ahead] = scores(*units[n + ahead])
        p[n] = probs(s.pop(n), i)
        if n >= behind:
            out(*units[n - behind], p.pop(n - behind))
    for n in sorted(p):
        out(*units[n], p[n])


def attend_call(qkv, heads):
    _, b, s, cq = qkv.shape
    return pl.pallas_call(
        functools.partial(attend_body, heads=heads, scale=128 ** -0.5), grid=(b,),
        in_specs=[pl.BlockSpec((4, 1, s, cq), lambda i: (0, i, 0, 0))],
        out_specs=pl.BlockSpec((4, 1, s, heads * 128), lambda i: (0, i, 0, 0)),
        out_shape=jax.ShapeDtypeStruct((4, b, s, heads * 128), BF),
        compiler_params=pltpu.CompilerParams(vmem_limit_bytes=VMEM_LIMIT), name="attend")(qkv)


def leave_body(c_ref, h_ref, wo_ref, wd_ref, x_ref, y_ref, out_ro, out_sib, out_rs, in_ro, in_sib, in_rs,
               lhs, w, stage, ra, rb, xs, l_sem, w_sem, st_sem, a_sem, s_ro, r_ro, s_rs, r_rs, s_sib, r_sib, *, M, T):
    LAG, CHUNK = 3, 384
    t, sib, far, far_sib = neighbours()
    meet(sib, far)
    kc, kh = c_ref.shape[2], h_ref.shape[2]
    N = wd_ref.shape[1] // T
    W = N // 2

    def w_copies(j, slot, width):
        cols = pl.ds(0, width)
        return (pltpu.make_async_copy(wo_ref.at[:, ds(j, width)], w.at[slot, pl.ds(0, kc), cols], w_sem.at[slot, 0]),
                pltpu.make_async_copy(wd_ref.at[:, ds(j, width)], w.at[slot, pl.ds(kc, kh), cols], w_sem.at[slot, 1]))

    pos_of = {"own": t, "sib": sib, "rs": far, "ro": far_sib}
    rel_of = {"own": 0, "sib": 1, "rs": 2, "ro": 3}

    def l_copies(kind, k, slot):
        return (pltpu.make_async_copy(c_ref.at[pos_of[kind], ds(k, M), :], lhs.at[slot, :, pl.ds(0, kc)], l_sem.at[slot, 0]),
                pltpu.make_async_copy(h_ref.at[rel_of[kind], ds(k, M), :], lhs.at[slot, :, pl.ds(kc, kh)], l_sem.at[slot, 1]))

    def start(cps):
        for cp in cps:
            cp.start()

    def wait(cps):
        for cp in cps:
            cp.wait()

    def remote(kind, i):
        src, dst, ss, rs, peer = {"ro": (out_ro, in_ro, s_ro, r_ro, sib), "sib": (out_sib, in_sib, s_sib, r_sib, sib),
                                  "rs": (out_rs, in_rs, s_rs, r_rs, far)}[kind]
        return send(src.at[i], dst.at[i], ss.at[i], rs.at[i], peer)

    def put(kind, i, slot):
        if kind == "own":
            return pltpu.make_async_copy(stage.at[slot], y_ref.at[ds(i // W, M), ds(lax.rem(i, W), 2 * T)], st_sem.at[slot])
        if kind == "sib":
            return pltpu.make_async_copy(stage.at[slot], out_sib.at[i], st_sem.at[slot])
        return pltpu.make_async_copy(stage.at[slot, :, pl.ds(0, T)], (out_ro if kind == "ro" else out_rs).at[i],
                                     st_sem.at[slot])

    def pass_on(kind, i, slot):
        put(kind, i, slot).wait()
        if kind != "own":
            remote(kind, i).start()

    def adds(kind, i, slot):
        if kind == "rs":
            return (pltpu.make_async_copy(in_ro.at[i], ra.at[slot, :, pl.ds(0, T)], a_sem.at[slot, 0]),)
        if kind == "own":
            return (pltpu.make_async_copy(in_sib.at[i], ra.at[slot], a_sem.at[slot, 0]),
                    pltpu.make_async_copy(in_rs.at[2 * i], rb.at[slot, :, pl.ds(0, T)], a_sem.at[slot, 1]),
                    pltpu.make_async_copy(in_rs.at[2 * i + 1], rb.at[slot, :, pl.ds(T, T)], a_sem.at[slot, 2]),
                    pltpu.make_async_copy(x_ref.at[ds(i // W, M), ds(lax.rem(i, W), 2 * T)], xs.at[slot], a_sem.at[slot, 3]))
        return ()

    def fetch(kind, i, slot):
        if kind == "rs":
            remote("ro", i).wait_recv()
        if kind == "own":
            remote("sib", i).wait_recv()
            remote("rs", 2 * i).wait_recv()
            remote("rs", 2 * i + 1).wait_recv()
        start(adds(kind, i, slot))
        if kind in ("ro", "rs"):
            start(w_copies(lax.rem(i, N), slot, T))
        else:
            start(w_copies(lax.rem(i, W), slot, 2 * T))

    def product(kind, i, ls, slot):
        wait(adds(kind, i, slot))
        cols = T if kind in ("ro", "rs") else 2 * T
        for r in range(0, M, CHUNK):
            rows = slice(r, r + CHUNK)
            z = jnp.dot(lhs[ls, rows], w[slot, :, 0:cols], preferred_element_type=F32)
            if kind == "rs":
                z = z + ra[slot, rows, 0:cols].astype(F32)
            if kind == "own":
                z = (z + ra[slot, rows].astype(F32)) + rb[slot, rows].astype(F32)
                z = xs[slot, rows].astype(F32) + z.astype(BF).astype(F32)
            stage[slot, rows, 0:cols] = z.astype(BF)

    fetch("ro", 0, 0)
    start(l_copies("ro", 0, 0))
    start(l_copies("rs", 0, 1))
    last = 2 * N - 1

    def far_rows(i, _):
        ro_slot = jnp.where(i < LAG, lax.rem(i, 2), LAG % 2)
        rs_slot = jnp.where(i <= last, 1 - LAG % 2, lax.rem(1 - LAG % 2 + i - last, 2))
        r = i - LAG

        @pl.when(i <= last)
        def _():
            @pl.when(lax.rem(i, N) == 0)
            def _():
                wait(l_copies("ro", 0, 0))
            wait(w_copies(0, ro_slot, T))

            @pl.when(i < LAG)
            def _():
                fetch("ro", i + 1, 1 - ro_slot)

            @pl.when(i >= LAG)
            def _():
                fetch("rs", r, 1 - ro_slot)
            product("ro", i, 0, ro_slot)

            @pl.when((i > 0) & (i <= LAG))
            def _():
                pass_on("ro", i - 1, 1 - ro_slot)

            @pl.when(i > LAG)
            def _():
                pass_on("rs", r - 1, 1 - ro_slot)
            put("ro", i, ro_slot).start()

            @pl.when(i == N - 1)
            def _():
                start(l_copies("ro", 1, 0))

        @pl.when(i >= LAG)
        def _():
            @pl.when(lax.rem(r, N) == 0)
            def _():
                wait(l_copies("rs", 0, 1))
            wait(w_copies(0, rs_slot, T))

            @pl.when(i < last)
            def _():
                fetch("ro", i + 1, 1 - rs_slot)

            @pl.when((i >= last) & (r < last))
            def _():
                fetch("rs", r + 1, 1 - rs_slot)

            @pl.when(r == last)
            def _():
                fetch("sib", 0, 1 - rs_slot)

            @pl.when(i == last)
            def _():
                start(l_copies("sib", 0, 0))
            product("rs", r, 1, rs_slot)

            @pl.when(i <= last)
            def _():
                pass_on("ro", i, 1 - rs_slot)

            @pl.when(i > last)
            def _():
                pass_on("rs", r - 1, 1 - rs_slot)
            put("rs", r, rs_slot).start()

            @pl.when(r == N - 1)
            def _():
                start(l_copies("rs", 1, 1))

            @pl.when(r == last)
            def _():
                start(l_copies("sib", 1, 1))
        return 0

    lax.fori_loop(0, last + 1 + LAG, far_rows, 0)
    end_slot = (1 - LAG % 2 + LAG) % 2
    base = 1 - end_slot

    def near_rows(kind, before):
        def step(i, _):
            k, slot = i // W, lax.rem(i + base, 2)

            @pl.when(lax.rem(i, W) == 0)
            def _():
                wait(l_copies(kind, 0, k))
            wait(w_copies(0, slot, 2 * T))

            @pl.when(i < 2 * W - 1)
            def _():
                fetch(kind, i + 1, 1 - slot)

            if kind == "sib":
                @pl.when(i == 2 * W - 1)
                def _():
                    fetch("own", 0, 1 - slot)

                @pl.when(i == W)
                def _():
                    start(l_copies("own", 0, 0))
            product(kind, i, k, slot)

            @pl.when(i == 0)
            def _():
                pass_on(before, last if before == "rs" else 2 * W - 1, 1 - slot)

            @pl.when(i > 0)
            def _():
                pass_on(kind, i - 1, 1 - slot)
            put(kind, i, slot).start()
            return 0

        lax.fori_loop(0, 2 * W, step, 0)

    near_rows("sib", "rs")
    start(l_copies("own", 1, 1))
    near_rows("own", "sib")
    put("own", 2 * W - 1, (2 * W - 1 + base) % 2).wait()

    def drain(i, _):
        remote("ro", i).wait_send()
        remote("rs", i).wait_send()

        @pl.when(i < 2 * W)
        def _():
            remote("sib", i).wait_send()
        return 0

    lax.fori_loop(0, 2 * N, drain, 0)


def leave_call(ctx, h, wo, wd, x):
    rows, d = x.shape
    M, T = rows // 2, 512
    N = d // T
    K = ctx.shape[2] + h.shape[2]
    dma = pltpu.SemaphoreType.DMA
    thin, wide = jax.ShapeDtypeStruct((2 * N, M, T), BF), jax.ShapeDtypeStruct((N, M, 2 * T), BF)
    out = pl.pallas_call(
        functools.partial(leave_body, M=M, T=T),
        in_specs=[ANY] * 5, out_specs=[ANY] * 7,
        out_shape=[jax.ShapeDtypeStruct((rows, d), BF), thin, wide, thin, thin, wide, thin],
        scratch_shapes=[pltpu.VMEM((2, M, K), BF), pltpu.VMEM((2, K, 2 * T), BF)] + [pltpu.VMEM((2, M, 2 * T), BF)] * 4
        + [dma((2, 2)), dma((2, 2)), dma((2,)), dma((2, 4))] + [dma((2 * N,))] * 4 + [dma((N,))] * 2,
        compiler_params=pltpu.CompilerParams(collective_id=1, has_side_effects=True, vmem_limit_bytes=VMEM_LIMIT),
        name="leave")(ctx, h, wo, wd, x)
    return out[0]


def solution(mesh):
    def local_layer(x_blk, ln_gain, ln_bias, w_qkv, w_out, w_up, w_down):
        b, s, d = x_blk.shape
        heads = w_qkv.shape[1]
        x = x_blk.reshape(b * s, d)
        qkv, h = enter_call(x, ln_gain.reshape(1, d), ln_bias.reshape(1, d), w_qkv.transpose(1, 2, 0, 3).reshape(heads * 3, d, 128), w_up)
        ctx = attend_call(qkv.reshape(4, b, s, -1), heads)
        y = leave_call(ctx.reshape(4, b * s, -1), h, w_out, w_down, x)
        return y.reshape(b, s, d)

    return jax.shard_map(
        local_layer, mesh=mesh,
        in_specs=(P("dp", "tp", None), P(), P(), P(None, "tp", None, None),
                  P("tp", None), P(None, "tp"), P("tp", None)),
        out_specs=P("dp", "tp", None), check_vma=False)
```
